32 devices in a mesh: floor: 4 (over y, x), zone: 8 (over z, core).
Axes of the slice: x: 2, y: 2, z: 4, core: 2. Of those that a mesh axis runs over, the one named last changes fastest.
Arguments:
- factor: float32 [512, 96, 384], P(('floor', 'zone')), may hold values from -0.625 to 0.625
- plant_map: float32 [512, 96, 384], P(('floor', 'zone')), may hold values from -0.4082483 to 0.4082483
- offset: float32 [512, 384], P(('floor', 'zone')), may hold values from -10 to 10
- start_plan: float32 [512, 384], P(('floor', 'zone')), may hold values from -10 to 10
- demand: float32 [4, 48], replicated, may hold values from -768 to 768
- start_price: float32 [4, 48], replicated, may hold values from -6 to 6
- start_multiplier: float32 [512, 48], P(('floor', 'zone')), may hold values from -6 to 6
- neighbors: int32 [512, 4], P(('floor', 'zone')), may hold values from 0 to 127
- loop_of_zone: int32 [512], P(('floor', 'zone')), may hold values from 0 to 3
Outputs:
- control: float32 [512, 384], P(('floor', 'zone'))
- price: float32 [4, 48], replicated
- multiplier: float32 [512, 48], P(('floor', 'zone'))
The draws below stay inside these ranges and needn't reach their ends.
Inputs may be any that keep to these rules, and one draw needn't show every extreme that they name: `neighbors`: indices count zones within the zone's own floor of 128 consecutive zones.
All inputs are finite; a program needn't handle non-finite values.
Results may differ from the reference program's by a relative error of at most 0.0001.
Values sent between devices are 32-bit elements; how exact they have to be, the bound alone decides.
A program may use at most 64 MiB of HBM per device.

```python
import math
import jax
import jax.numpy as jnp
from jax import lax

HORIZON = 48
NEIGHBORS = 4
LOOPS = 4
ITERS = 2
CONTROLS = 384
FLOOR_ZONES = 128
ZONES = 512


def common_parts(key):
    base = jax.random.fold_in(key, 5171)
    key_map, key_plan = jax.random.split(base)
    map_scale = 1.0 / math.sqrt(CONTROLS)
    shared_map = jnp.clip(jax.random.normal(key_map, (HORIZON, CONTROLS), jnp.float32), -4.0, 4.0) * map_scale
    shared_plan = jnp.clip(jax.random.normal(key_plan, (CONTROLS,), jnp.float32), -4.0, 4.0)
    return (shared_map, shared_plan)


def zone_noise(key, shape):
    return jnp.clip(jax.random.normal(key, shape, jnp.float32), -4.0, 4.0)


def draw_plant_map(key, part):
    shared_map, shared_plan = common_parts(key)
    own_key = jax.random.fold_in(key, 5172)
    map_scale = 1.0 / math.sqrt(CONTROLS)
    noise = zone_noise(own_key, (ZONES, 2 * HORIZON, CONTROLS)) * map_scale
    head = noise[:, :HORIZON, :] + shared_map[None, :, :]
    return jnp.concatenate([head, noise[:, HORIZON:, :]], axis=1).astype(jnp.float32)


def draw_start_plan(key, part):
    shared_map, shared_plan = common_parts(key)
    own_key = jax.random.fold_in(key, 5173)
    noise = zone_noise(own_key, (ZONES, CONTROLS))
    return (shared_plan[None, :] + noise).astype(jnp.float32)


def draw_offset(key, part):
    shared_map, shared_plan = common_parts(key)
    own_key = jax.random.fold_in(key, 5174)
    noise = zone_noise(own_key, (ZONES, CONTROLS))
    return (noise - shared_plan[None, :]).astype(jnp.float32)


def plant(values, key, least, top_value):
    dims = values.shape
    index_at = [jax.random.randint(jax.random.fold_in(key, axis), (), 0, dims[axis]) for axis in range(len(dims))]
    values = values.at[tuple(index_at)].set(least)
    longest = dims.index(max(dims))
    index_at[longest] = (index_at[longest] + 1) % dims[longest]
    return values.at[tuple(index_at)].set(top_value)


def block_scale(key, dims, cuts, smallest, largest):
    factor_of = 1.0
    for position, shards_of in cuts:
        draws = jax.random.uniform(jax.random.fold_in(jax.random.fold_in(key, 6), position), (shards_of,), jnp.float32, smallest / len(cuts), largest / len(cuts))
        factor_of = factor_of * jnp.repeat(jnp.exp(draws), dims[position] // shards_of).reshape((-1,) + (1,) * (len(dims) - 1 - position))
    return factor_of


def bell_draw(key, shape, width, limit, shards=(), kind=jnp.bfloat16):
    drawn = width * jax.random.normal(key, shape, jnp.float32)
    if shards:
        drawn = drawn * block_scale(key, shape, shards, -0.22, 0.18)
    return jnp.clip(drawn, -limit, limit).astype(kind)


def setup_inputs(seed: int = 0) -> dict:
    splits = jax.random.split(jax.random.key(seed), 10)
    return {
        "factor": bell_draw(splits[0], (ZONES, 2 * HORIZON, CONTROLS), (2 * HORIZON) ** -0.5, 0.625, ((0, 32),), jnp.float32),
        "plant_map": draw_plant_map(jax.random.fold_in(splits[9], 71), 0),
        "offset": draw_offset(jax.random.fold_in(splits[9], 71), 0),
        "start_plan": draw_start_plan(jax.random.fold_in(splits[9], 71), 0),
        "demand": bell_draw(splits[4], (LOOPS, HORIZON), (ZONES // LOOPS), 768.0, (), jnp.float32),
        "start_price": bell_draw(splits[5], (LOOPS, HORIZON), 1.0, 6.0, (), jnp.float32),
        "start_multiplier": bell_draw(splits[6], (ZONES, HORIZON), 1.0, 6.0, ((0, 32),), jnp.float32),
        "neighbors": plant(jax.random.randint(splits[7], (ZONES, NEIGHBORS), 0, FLOOR_ZONES), jax.random.fold_in(splits[7], 1), 0, FLOOR_ZONES - 1).astype(jnp.int32),
        "loop_of_zone": plant(jax.random.randint(splits[8], (ZONES,), 0, LOOPS), jax.random.fold_in(splits[8], 1), 0, LOOPS - 1).astype(jnp.int32),
    }


def reference(factor, plant_map, offset, start_plan, demand, start_price, start_multiplier, neighbors, loop_of_zone):
    control = start_plan
    price = start_price
    multiplier = start_multiplier
    onehot = (loop_of_zone[:, None] == jnp.arange(LOOPS, dtype=jnp.int32)[None, :]).astype(jnp.float32)
    floor_base = (jnp.arange(ZONES, dtype=jnp.int32) // FLOOR_ZONES) * FLOOR_ZONES
    global_index = (floor_base[:, None] + neighbors).astype(jnp.int32)
    for step in range(ITERS):
        outputs = jnp.einsum("zkv,zv->zk", plant_map, control, precision=lax.Precision.HIGHEST)
        shares = outputs[:, :HORIZON]
        bound = outputs[:, HORIZON:]
        total = jnp.dot(onehot.T, shares, precision=lax.Precision.HIGHEST)
        excess = (total - demand) * (LOOPS / ZONES)
        shift = jnp.dot(onehot, excess + price, precision=lax.Precision.HIGHEST)
        price = price + excess
        target_share = shares - shift
        near = jnp.mean(bound[global_index], axis=1)
        target_bound = (bound + near) / 2.0 - multiplier
        multiplier = multiplier + (bound - near) / 2.0
        target = jnp.concatenate([target_share, target_bound], axis=1)
        control = 0.8 * jnp.einsum("zkv,zk->zv", factor, target, precision=lax.Precision.HIGHEST) - offset
    return control, price, multiplier
```

```python
import functools

import jax
import jax.numpy as jnp
from jax import lax
from jax.experimental import pallas as pl
from jax.experimental.pallas import tpu as pltpu
from jax.sharding import PartitionSpec as P

ITERS = 2
MESH = pl.DeviceIdType.MESH
SUB, LANE = 8, 128
CHUNKS = 4


def pieces(x):
    high = x.astype(jnp.bfloat16)
    rest = x - high.astype(jnp.float32)
    mid = rest.astype(jnp.bfloat16)
    low = rest - mid.astype(jnp.float32)
    zero = jnp.zeros_like(low)
    return jnp.concatenate(
        [high.astype(jnp.float32), mid.astype(jnp.float32), low, zero], axis=0
    ).astype(jnp.bfloat16)


def exact_dot(x, picks):
    parts = jnp.dot(pieces(x), picks, preferred_element_type=jnp.float32)
    return parts[:SUB] + parts[SUB : 2 * SUB] + parts[2 * SUB : 3 * SUB]


def kernel(
    floors,
    cols,
    zones_all,
    factor_ref,
    plant_ref,
    offset_ref,
    plan_ref,
    demand_ref,
    price_ref,
    mult_ref,
    near_ref,
    loop_ref,
    control_out,
    price_out,
    mult_out,
    factor,
    plant,
    control,
    select,
    message,
    heard,
    floor_message,
    floor_heard,
    plant_sem,
    factor_sem,
    send_sem,
    recv_sem,
    floor_send_sem,
    floor_recv_sem,
):
    zones, rows, width = plant.shape
    horizon = rows // 2
    groups = horizon // SUB
    loops = demand_ref.shape[0]
    base = groups * zones
    my_floor, me = lax.axis_index("floor"), lax.axis_index("zone")

    step_zones = zones // CHUNKS
    plant_copies, factor_copies = [], []
    for i in range(CHUNKS):
        part = pl.ds(i * step_zones, step_zones)
        plant_copies.append(pltpu.make_async_copy(plant_ref.at[part], plant.at[part], plant_sem.at[i]))
        factor_copies.append(
            pltpu.make_async_copy(factor_ref.at[part], factor.at[part], factor_sem.at[i])
        )
    for copy in plant_copies + factor_copies:
        copy.start()

    zone_peers = [(my_floor, lax.rem(me + d, cols)) for d in range(1, cols)]
    floor_peers = [(lax.rem(my_floor + d, floors), me) for d in range(1, floors)]
    barrier = pltpu.get_barrier_semaphore()
    for peer in zone_peers + floor_peers:
        pl.semaphore_signal(barrier, inc=1, device_id=peer, device_id_type=MESH)

    lane = lax.broadcasted_iota(jnp.int32, (SUB, LANE), 1)

    def pack(x, start):
        count = x.shape[0]
        row = lax.broadcasted_iota(jnp.int32, (count, LANE), 0)
        col = lax.broadcasted_iota(jnp.int32, (count, LANE), 1) - start
        inside = (col >= 0) & (col < groups * count)
        spread = ((lax.rem(jnp.maximum(col, 0), count) == row) & inside).astype(jnp.float32)
        wide = lax.dot_general(
            x, spread, (((0,), (0,)), ((), ())),
            precision=lax.Precision.HIGHEST, preferred_element_type=jnp.float32,
        )
        out = jnp.zeros((SUB, LANE), jnp.float32)
        for j in range(groups):
            first = start + count * j
            mine = (lane >= first) & (lane < first + count)
            out = jnp.where(mine, wide[SUB * j : SUB * (j + 1)], out)
        return out

    def unpack(tile, count, start):
        row = lax.broadcasted_iota(jnp.int32, (count, LANE), 0)
        col = lax.broadcasted_iota(jnp.int32, (count, LANE), 1) - start
        inside = (col >= 0) & (col < groups * count)
        spread = ((lax.rem(jnp.maximum(col, 0), count) == row) & inside).astype(jnp.float32)
        parts = []
        for j in range(groups):
            first = start + count * j
            mine = (lane >= first) & (lane < first + count)
            parts.append(jnp.where(mine, tile, 0.0))
        tall = jnp.concatenate(parts, axis=0)
        return lax.dot_general(
            spread, tall, (((1,), (1,)), ((), ())),
            precision=lax.Precision.HIGHEST, preferred_element_type=jnp.float32,
        )

    is_load = (lane >= base) & (lane < base + groups * loops)
    demand = pack(demand_ref[...], base)
    price = pack(price_ref[...], base)
    mult = pack(mult_ref[...], 0)

    row = lax.broadcasted_iota(jnp.int32, (LANE, LANE), 0)
    col = lax.broadcasted_iota(jnp.int32, (LANE, LANE), 1)
    wide_lane = lax.broadcasted_iota(jnp.int32, (1, LANE), 1)
    lane_zone = lax.rem(wide_lane, zones)
    same = (row // zones == col // zones) & (row < base) & (col < base)
    count = near_ref.shape[1]
    names = []
    for b in range(count):
        value = jnp.zeros((1, LANE), jnp.int32)
        for z in range(zones):
            value = jnp.where(lane_zone == z, near_ref[z, b], value)
        names.append(jnp.broadcast_to(value, (LANE, LANE)))
    inner = lax.rem(row, zones)
    for d in range(cols):
        owner = lax.rem(me - d + cols, cols)
        target = inner + owner * zones
        hits = jnp.zeros((LANE, LANE), jnp.float32)
        for b in range(count):
            hits += (names[b] == target).astype(jnp.float32)
        select[d * LANE : (d + 1) * LANE, :] = jnp.where(same, hits / count, 0.0).astype(jnp.bfloat16)
    loop_lane = jnp.zeros((1, LANE), jnp.int32)
    for z in range(zones):
        loop_lane = jnp.where(lane_zone == z, loop_ref[z], loop_lane)
    wanted = base + (col // zones) * loops + jnp.broadcast_to(loop_lane, (LANE, LANE))
    loop_pick = ((row == wanted) & (col < base)).astype(jnp.float32).astype(jnp.bfloat16)

    loop_of = [loop_ref[z] for z in range(zones)]
    slots = cols - 1
    floor_slots = floors - 1
    sends = []
    for step in range(ITERS):
        source = plan_ref if step == 0 else control
        shares = jnp.zeros((SUB, LANE), jnp.float32)
        tile = jnp.zeros((SUB, LANE), jnp.float32)
        loads = jnp.zeros((SUB, LANE), jnp.float32)
        for z in range(zones):
            if step == 0 and z % step_zones == 0:
                plant_copies[z // step_zones].wait()
            product = plant[z] * source[z : z + 1, :]
            partial = product[:, :LANE]
            for c in range(1, width // LANE):
                partial += product[:, c * LANE : (c + 1) * LANE]
            sums = jnp.sum(partial, axis=1, keepdims=True)
            for j in range(groups):
                share = jnp.broadcast_to(sums[SUB * j : SUB * (j + 1)], (SUB, LANE))
                first = horizon + SUB * j
                bound = jnp.broadcast_to(sums[first : first + SUB], (SUB, LANE))
                mine = lane == zones * j + z
                shares = jnp.where(mine, share, shares)
                tile = jnp.where(mine, bound, tile)
                loads += jnp.where(lane == base + loops * j + loop_of[z], share, 0.0)
        tile = tile + loads
        message[step] = tile
        if step == 0:
            pl.semaphore_wait(barrier, slots + floor_slots)
        for d in range(1, cols):
            copy = pltpu.make_async_remote_copy(
                src_ref=message.at[step],
                dst_ref=heard.at[step, d - 1],
                send_sem=send_sem.at[step, d - 1],
                recv_sem=recv_sem.at[step, d - 1],
                device_id=zone_peers[d - 1],
                device_id_type=MESH,
            )
            copy.start()
            sends.append(copy)
        for copy in sends[len(sends) - slots :]:
            copy.wait_recv()
        floor_tile = tile
        for d in range(slots):
            floor_tile += heard[step, d]
        floor_message[step] = floor_tile
        floor_sends = []
        for d in range(1, floors):
            copy = pltpu.make_async_remote_copy(
                src_ref=floor_message.at[step],
                dst_ref=floor_heard.at[step, d - 1],
                send_sem=floor_send_sem.at[step, d - 1],
                recv_sem=floor_recv_sem.at[step, d - 1],
                device_id=floor_peers[d - 1],
                device_id_type=MESH,
            )
            copy.start()
            floor_sends.append(copy)
        everyone = jnp.concatenate([tile] + [heard[step, d] for d in range(slots)], axis=1)
        near = exact_dot(everyone, select[...])
        here = jnp.where(lane < base, tile, 0.0)
        target_bound = (here + near) * 0.5 - mult
        mult = mult + (here - near) * 0.5
        for copy in floor_sends:
            copy.wait_recv()
        sends += floor_sends
        total = floor_tile
        for d in range(floor_slots):
            total += floor_heard[step, d]
        excess = jnp.where(is_load, (total - demand) * (loops / zones_all), 0.0)
        target_share = shares - exact_dot(excess + price, loop_pick)
        price = price + excess
        for z in range(zones):
            if step == 0 and z % step_zones == 0:
                factor_copies[z // step_zones].wait()
            total_z = jnp.zeros((SUB, width), jnp.float32)
            for half, target in enumerate((target_share, target_bound)):
                for j in range(groups):
                    at = zones * j + z
                    column = jnp.broadcast_to(target[:, at : at + 1], (SUB, width))
                    first = half * horizon + SUB * j
                    total_z += factor[z, first : first + SUB, :] * column
            result = 0.8 * jnp.sum(total_z, axis=0, keepdims=True) - offset_ref[z : z + 1, :]
            if step == ITERS - 1:
                control_out[z : z + 1, :] = result
            else:
                control[z : z + 1, :] = result
    price_out[...] = unpack(price, loops, base)
    mult_out[...] = unpack(mult, zones, 0)
    for copy in sends:
        copy.wait_send()


def solution(mesh):
    floors, cols = mesh.shape["floor"], mesh.shape["zone"]

    def local(factor, plant, offset, plan, demand, price, mult, near, loop):
        zones = plan.shape[0]
        assert (zones + loop_count(demand)) * demand.shape[1] // SUB <= LANE
        vmem, smem = pl.BlockSpec(memory_space=pltpu.VMEM), pl.BlockSpec(memory_space=pltpu.SMEM)
        anywhere = pl.BlockSpec(memory_space=pl.ANY)
        dma = pltpu.SemaphoreType.DMA
        tile = (SUB, LANE)
        return pl.pallas_call(
            functools.partial(kernel, floors, cols, zones * floors * cols),
            out_shape=tuple(jax.ShapeDtypeStruct(x.shape, x.dtype) for x in (plan, price, mult)),
            in_specs=[anywhere, anywhere, vmem, vmem, vmem, vmem, vmem, smem, smem],
            out_specs=(vmem, vmem, vmem),
            scratch_shapes=[
                pltpu.VMEM(factor.shape, jnp.float32),
                pltpu.VMEM(plant.shape, jnp.float32),
                pltpu.VMEM(plan.shape, jnp.float32),
                pltpu.VMEM((cols * LANE, LANE), jnp.bfloat16),
                pltpu.VMEM((ITERS,) + tile, jnp.float32),
                pltpu.VMEM((ITERS, cols - 1) + tile, jnp.float32),
                pltpu.VMEM((ITERS,) + tile, jnp.float32),
                pltpu.VMEM((ITERS, floors - 1) + tile, jnp.float32),
                dma((CHUNKS,)),
                dma((CHUNKS,)),
                dma((ITERS, cols - 1)),
                dma((ITERS, cols - 1)),
                dma((ITERS, floors - 1)),
                dma((ITERS, floors - 1)),
            ],
            compiler_params=pltpu.CompilerParams(collective_id=0, has_side_effects=True),
        )(factor, plant, offset, plan, demand, price, mult, near, loop)

    def loop_count(demand):
        return demand.shape[0]

    both = ("floor", "zone")
    placed = (
        P(both, None, None), P(both, None, None), P(both, None), P(both, None),
        P(), P(), P(both, None), P(both, None), P(both),
    )
    return jax.shard_map(
        local,
        mesh=mesh,
        in_specs=placed,
        out_specs=(P(both, None), P(), P(both, None)),
        check_vma=False,
    )
```

```python
import functools

import jax
import jax.numpy as jnp
from jax import lax
from jax.experimental import pallas as pl
from jax.experimental.pallas import tpu as pltpu
from jax.sharding import PartitionSpec as P

ITERS = 2
MESH = pl.DeviceIdType.MESH
SUB, LANE = 8, 128
CHUNKS = 4


def pieces(x):
    high = x.astype(jnp.bfloat16)
    rest = x - high.astype(jnp.float32)
    mid = rest.astype(jnp.bfloat16)
    low = rest - mid.astype(jnp.float32)
    zero = jnp.zeros_like(low)
    return jnp.concatenate(
        [high.astype(jnp.float32), mid.astype(jnp.float32), low, zero], axis=0
    ).astype(jnp.bfloat16)


def exact_dot(x, picks):
    parts = jnp.dot(pieces(x), picks, preferred_element_type=jnp.float32)
    return parts[:SUB] + parts[SUB : 2 * SUB] + parts[2 * SUB : 3 * SUB]


def kernel(
    floors,
    cols,
    zones_all,
    factor_ref,
    plant_ref,
    offset_ref,
    plan_ref,
    demand_ref,
    price_ref,
    mult_ref,
    near_ref,
    loop_ref,
    control_out,
    price_out,
    mult_out,
    factor,
    plant,
    control,
    select,
    message,
    heard,
    floor_message,
    floor_heard,
    plant_sem,
    factor_sem,
    send_sem,
    recv_sem,
    floor_send_sem,
    floor_recv_sem,
):
    zones, rows, width = plant.shape
    horizon = rows // 2
    groups = horizon // SUB
    loops = demand_ref.shape[0]
    base = groups * zones
    my_floor, me = lax.axis_index("floor"), lax.axis_index("zone")

    step_zones = zones // CHUNKS
    plant_copies, factor_copies = [], []
    for i in range(CHUNKS):
        part = pl.ds(i * step_zones, step_zones)
        plant_copies.append(pltpu.make_async_copy(plant_ref.at[part], plant.at[part], plant_sem.at[i]))
        factor_copies.append(
            pltpu.make_async_copy(factor_ref.at[part], factor.at[part], factor_sem.at[i])
        )
    for copy in plant_copies + factor_copies:
        copy.start()

    zone_peers = [(my_floor, lax.rem(me + d, cols)) for d in range(1, cols)]
    floor_peers = [(lax.rem(my_floor + d, floors), me) for d in range(1, floors)]
    barrier = pltpu.get_barrier_semaphore()
    for peer in zone_peers + floor_peers:
        pl.semaphore_signal(barrier, inc=1, device_id=peer, device_id_type=MESH)

    lane = lax.broadcasted_iota(jnp.int32, (SUB, LANE), 1)

    def pack(x, start):
        count = x.shape[0]
        row = lax.broadcasted_iota(jnp.int32, (count, LANE), 0)
        col = lax.broadcasted_iota(jnp.int32, (count, LANE), 1) - start
        inside = (col >= 0) & (col < groups * count)
        spread = ((lax.rem(jnp.maximum(col, 0), count) == row) & inside).astype(jnp.float32)
        wide = lax.dot_general(
            x, spread, (((0,), (0,)), ((), ())),
            precision=lax.Precision.HIGHEST, preferred_element_type=jnp.float32,
        )
        out = jnp.zeros((SUB, LANE), jnp.float32)
        for j in range(groups):
            first = start + count * j
            mine = (lane >= first) & (lane < first + count)
            out = jnp.where(mine, wide[SUB * j : SUB * (j + 1)], out)
        return out

    def unpack(tile, count, start):
        row = lax.broadcasted_iota(jnp.int32, (count, LANE), 0)
        col = lax.broadcasted_iota(jnp.int32, (count, LANE), 1) - start
        inside = (col >= 0) & (col < groups * count)
        spread = ((lax.rem(jnp.maximum(col, 0), count) == row) & inside).astype(jnp.float32)
        parts = []
        for j in range(groups):
            first = start + count * j
            mine = (lane >= first) & (lane < first + count)
            parts.append(jnp.where(mine, tile, 0.0))
        tall = jnp.concatenate(parts, axis=0)
        return lax.dot_general(
            spread, tall, (((1,), (1,)), ((), ())),
            precision=lax.Precision.HIGHEST, preferred_element_type=jnp.float32,
        )

    is_load = (lane >= base) & (lane < base + groups * loops)
    demand = pack(demand_ref[...], base)
    price = pack(price_ref[...], base)
    mult = pack(mult_ref[...], 0)

    row = lax.broadcasted_iota(jnp.int32, (LANE, LANE), 0)
    col = lax.broadcasted_iota(jnp.int32, (LANE, LANE), 1)
    wide_lane = lax.broadcasted_iota(jnp.int32, (1, LANE), 1)
    lane_zone = lax.rem(wide_lane, zones)
    same = (row // zones == col // zones) & (row < base) & (col < base)
    count = near_ref.shape[0]
    names = []
    for b in range(count):
        value = jnp.zeros((1, LANE), jnp.int32)
        for z in range(zones):
            value = jnp.where(lane_zone == z, near_ref[b, z], value)
        names.append(jnp.broadcast_to(value, (LANE, LANE)))
    inner = lax.rem(row, zones)
    for d in range(cols):
        owner = lax.rem(me - d + cols, cols)
        target = inner + owner * zones
        hits = jnp.zeros((LANE, LANE), jnp.float32)
        for b in range(count):
            hits += (names[b] == target).astype(jnp.float32)
        select[d * LANE : (d + 1) * LANE, :] = jnp.where(same, hits / count, 0.0).astype(jnp.bfloat16)
    loop_lane = jnp.zeros((1, LANE), jnp.int32)
    for z in range(zones):
        loop_lane = jnp.where(lane_zone == z, loop_ref[z], loop_lane)
    wanted = base + (col // zones) * loops + jnp.broadcast_to(loop_lane, (LANE, LANE))
    loop_pick = ((row == wanted) & (col < base)).astype(jnp.float32).astype(jnp.bfloat16)

    loop_of = [loop_ref[z] for z in range(zones)]
    slots = cols - 1
    floor_slots = floors - 1
    sends = []
    for step in range(ITERS):
        source = plan_ref if step == 0 else control
        shares = jnp.zeros((SUB, LANE), jnp.float32)
        tile = jnp.zeros((SUB, LANE), jnp.float32)
        loads = jnp.zeros((SUB, LANE), jnp.float32)
        for z in range(zones):
            if step == 0 and z % step_zones == 0:
                plant_copies[z // step_zones].wait()
            product = plant[z] * source[z : z + 1, :]
            partial = product[:, :LANE]
            for c in range(1, width // LANE):
                partial += product[:, c * LANE : (c + 1) * LANE]
            sums = jnp.sum(partial, axis=1, keepdims=True)
            for j in range(groups):
                share = jnp.broadcast_to(sums[SUB * j : SUB * (j + 1)], (SUB, LANE))
                first = horizon + SUB * j
                bound = jnp.broadcast_to(sums[first : first + SUB], (SUB, LANE))
                mine = lane == zones * j + z
                shares = jnp.where(mine, share, shares)
                tile = jnp.where(mine, bound, tile)
                loads += jnp.where(lane == base + loops * j + loop_of[z], share, 0.0)
        tile = tile + loads
        message[step] = tile
        if step == 0:
            pl.semaphore_wait(barrier, slots + floor_slots)
        for d in range(1, cols):
            copy = pltpu.make_async_remote_copy(
                src_ref=message.at[step],
                dst_ref=heard.at[step, d - 1],
                send_sem=send_sem.at[step, d - 1],
                recv_sem=recv_sem.at[step, d - 1],
                device_id=zone_peers[d - 1],
                device_id_type=MESH,
            )
            copy.start()
            sends.append(copy)
        for copy in sends[len(sends) - slots :]:
            copy.wait_recv()
        floor_tile = tile
        for d in range(slots):
            floor_tile += heard[step, d]
        floor_message[step] = floor_tile
        floor_sends = []
        for d in range(1, floors):
            copy = pltpu.make_async_remote_copy(
                src_ref=floor_message.at[step],
                dst_ref=floor_heard.at[step, d - 1],
                send_sem=floor_send_sem.at[step, d - 1],
                recv_sem=floor_recv_sem.at[step, d - 1],
                device_id=floor_peers[d - 1],
                device_id_type=MESH,
            )
            copy.start()
            floor_sends.append(copy)
        everyone = jnp.concatenate([tile] + [heard[step, d] for d in range(slots)], axis=1)
        near = exact_dot(everyone, select[...])
        here = jnp.where(lane < base, tile, 0.0)
        target_bound = (here + near) * 0.5 - mult
        mult = mult + (here - near) * 0.5
        for copy in floor_sends:
            copy.wait_recv()
        sends += floor_sends
        total = floor_tile
        for d in range(floor_slots):
            total += floor_heard[step, d]
        excess = jnp.where(is_load, (total - demand) * (loops / zones_all), 0.0)
        target_share = shares - exact_dot(excess + price, loop_pick)
        price = price + excess
        for z in range(zones):
            if step == 0 and z % step_zones == 0:
                factor_copies[z // step_zones].wait()
            total_z = jnp.zeros((SUB, width), jnp.float32)
            for half, target in enumerate((target_share, target_bound)):
                for j in range(groups):
                    at = zones * j + z
                    column = jnp.broadcast_to(target[:, at : at + 1], (SUB, width))
                    first = half * horizon + SUB * j
                    total_z += factor[z, first : first + SUB, :] * column
            result = 0.8 * jnp.sum(total_z, axis=0, keepdims=True) - offset_ref[z : z + 1, :]
            if step == ITERS - 1:
                control_out[z : z + 1, :] = result
            else:
                control[z : z + 1, :] = result
    price_out[...] = unpack(price, loops, base)
    mult_out[...] = unpack(mult, zones, 0)
    for copy in sends:
        copy.wait_send()


def hand_over(*refs):
    for source, target in zip(refs[:3], refs[3:]):
        target[...] = source[...]


def solution(mesh):
    floors, cols = mesh.shape["floor"], mesh.shape["zone"]

    def local(factor, plant, offset, plan, demand, price, mult, near, loop):
        zones = plan.shape[0]
        assert (zones + loop_count(demand)) * demand.shape[1] // SUB <= LANE
        vmem, smem = pl.BlockSpec(memory_space=pltpu.VMEM), pl.BlockSpec(memory_space=pltpu.SMEM)
        anywhere = pl.BlockSpec(memory_space=pl.ANY)
        dma = pltpu.SemaphoreType.DMA
        tile = (SUB, LANE)
        results = pl.pallas_call(
            functools.partial(kernel, floors, cols, zones * floors * cols),
            out_shape=tuple(jax.ShapeDtypeStruct(x.shape, x.dtype) for x in (plan, price, mult)),
            in_specs=[anywhere, anywhere, vmem, vmem, vmem, vmem, vmem, smem, smem],
            out_specs=(vmem, vmem, vmem),
            scratch_shapes=[
                pltpu.VMEM(factor.shape, jnp.float32),
                pltpu.VMEM(plant.shape, jnp.float32),
                pltpu.VMEM(plan.shape, jnp.float32),
                pltpu.VMEM((cols * LANE, LANE), jnp.bfloat16),
                pltpu.VMEM((ITERS,) + tile, jnp.float32),
                pltpu.VMEM((ITERS, cols - 1) + tile, jnp.float32),
                pltpu.VMEM((ITERS,) + tile, jnp.float32),
                pltpu.VMEM((ITERS, floors - 1) + tile, jnp.float32),
                dma((CHUNKS,)),
                dma((CHUNKS,)),
                dma((ITERS, cols - 1)),
                dma((ITERS, cols - 1)),
                dma((ITERS, floors - 1)),
                dma((ITERS, floors - 1)),
            ],
            compiler_params=pltpu.CompilerParams(collective_id=0, has_side_effects=True),
        )(factor, plant, offset, plan, demand, price, mult, near.T, loop)
        return pl.pallas_call(
            hand_over,
            out_shape=tuple(jax.ShapeDtypeStruct(x.shape, x.dtype) for x in results),
            in_specs=[vmem] * 3,
            out_specs=(vmem,) * 3,
        )(*results)

    def loop_count(demand):
        return demand.shape[0]

    both = ("floor", "zone")
    placed = (
        P(both, None, None), P(both, None, None), P(both, None), P(both, None),
        P(), P(), P(both, None), P(both, None), P(both),
    )
    return jax.shard_map(
        local,
        mesh=mesh,
        in_specs=placed,
        out_specs=(P(both, None), P(), P(both, None)),
        check_vma=False,
    )
```

```python
import functools

import jax
import jax.numpy as jnp
from jax import lax
from jax.experimental import pallas as pl
from jax.experimental.pallas import tpu as pltpu
from jax.sharding import PartitionSpec as P

ITERS = 2
MESH = pl.DeviceIdType.MESH
SUB, LANE = 8, 128
CHUNKS = 4


def pieces(x):
    high = x.astype(jnp.bfloat16)
    rest = x - high.astype(jnp.float32)
    mid = rest.astype(jnp.bfloat16)
    low = rest - mid.astype(jnp.float32)
    zero = jnp.zeros_like(low)
    return jnp.concatenate(
        [high.astype(jnp.float32), mid.astype(jnp.float32), low, zero], axis=0
    ).astype(jnp.bfloat16)


def exact_dot(x, picks):
    parts = jnp.dot(pieces(x), picks, preferred_element_type=jnp.float32)
    return parts[:SUB] + parts[SUB : 2 * SUB] + parts[2 * SUB : 3 * SUB]


def kernel(
    floors,
    cols,
    zones_all,
    factor_ref,
    plant_ref,
    offset_hbm,
    plan_hbm,
    demand_hbm,
    price_hbm,
    mult_hbm,
    near_hbm,
    loop_hbm,
    control_out,
    price_out,
    mult_out,
    factor,
    plant,
    control,
    select,
    message,
    heard,
    floor_message,
    floor_heard,
    offset_ref,
    plan_ref,
    demand_ref,
    price_ref,
    mult_ref,
    near_ref,
    loop_ref,
    small_sem,
    plant_sem,
    factor_sem,
    send_sem,
    recv_sem,
    floor_send_sem,
    floor_recv_sem,
):
    zones, rows, width = plant.shape
    horizon = rows // 2
    groups = horizon // SUB
    loops = demand_ref.shape[0]
    base = groups * zones
    my_floor, me = lax.axis_index("floor"), lax.axis_index("zone")

    step_zones = zones // CHUNKS
    plant_copies, factor_copies = [], []
    for i in range(CHUNKS):
        part = pl.ds(i * step_zones, step_zones)
        plant_copies.append(pltpu.make_async_copy(plant_ref.at[part], plant.at[part], plant_sem.at[i]))
        factor_copies.append(
            pltpu.make_async_copy(factor_ref.at[part], factor.at[part], factor_sem.at[i])
        )
    sources = (loop_hbm, near_hbm, mult_hbm, demand_hbm, price_hbm, plan_hbm, offset_hbm)
    targets = (loop_ref, near_ref, mult_ref, demand_ref, price_ref, plan_ref, offset_ref)
    small = [
        pltpu.make_async_copy(source, target, small_sem.at[i])
        for i, (source, target) in enumerate(zip(sources, targets))
    ]
    for copy in small + plant_copies + factor_copies:
        copy.start()

    zone_peers = [(my_floor, lax.rem(me + d, cols)) for d in range(1, cols)]
    floor_peers = [(lax.rem(my_floor + d, floors), me) for d in range(1, floors)]
    barrier = pltpu.get_barrier_semaphore()
    for peer in zone_peers + floor_peers:
        pl.semaphore_signal(barrier, inc=1, device_id=peer, device_id_type=MESH)

    lane = lax.broadcasted_iota(jnp.int32, (SUB, LANE), 1)

    def pack(x, start):
        count = x.shape[0]
        row = lax.broadcasted_iota(jnp.int32, (count, LANE), 0)
        col = lax.broadcasted_iota(jnp.int32, (count, LANE), 1) - start
        inside = (col >= 0) & (col < groups * count)
        spread = ((lax.rem(jnp.maximum(col, 0), count) == row) & inside).astype(jnp.float32)
        wide = lax.dot_general(
            x, spread, (((0,), (0,)), ((), ())),
            precision=lax.Precision.HIGHEST, preferred_element_type=jnp.float32,
        )
        out = jnp.zeros((SUB, LANE), jnp.float32)
        for j in range(groups):
            first = start + count * j
            mine = (lane >= first) & (lane < first + count)
            out = jnp.where(mine, wide[SUB * j : SUB * (j + 1)], out)
        return out

    def unpack(tile, count, start):
        row = lax.broadcasted_iota(jnp.int32, (count, LANE), 0)
        col = lax.broadcasted_iota(jnp.int32, (count, LANE), 1) - start
        inside = (col >= 0) & (col < groups * count)
        spread = ((lax.rem(jnp.maximum(col, 0), count) == row) & inside).astype(jnp.float32)
        parts = []
        for j in range(groups):
            first = start + count * j
            mine = (lane >= first) & (lane < first + count)
            parts.append(jnp.where(mine, tile, 0.0))
        tall = jnp.concatenate(parts, axis=0)
        return lax.dot_general(
            spread, tall, (((1,), (1,)), ((), ())),
            precision=lax.Precision.HIGHEST, preferred_element_type=jnp.float32,
        )

    is_load = (lane >= base) & (lane < base + groups * loops)
    for copy in small:
        copy.wait()
    demand = pack(demand_ref[...], base)
    price = pack(price_ref[...], base)
    mult = pack(mult_ref[...], 0)

    row = lax.broadcasted_iota(jnp.int32, (LANE, LANE), 0)
    col = lax.broadcasted_iota(jnp.int32, (LANE, LANE), 1)
    wide_lane = lax.broadcasted_iota(jnp.int32, (1, LANE), 1)
    lane_zone = lax.rem(wide_lane, zones)
    same = (row // zones == col // zones) & (row < base) & (col < base)
    count = near_ref.shape[0]
    names = []
    for b in range(count):
        value = jnp.zeros((1, LANE), jnp.int32)
        for z in range(zones):
            value = jnp.where(lane_zone == z, near_ref[b, z], value)
        names.append(jnp.broadcast_to(value, (LANE, LANE)))
    inner = lax.rem(row, zones)
    for d in range(cols):
        owner = lax.rem(me - d + cols, cols)
        target = inner + owner * zones
        hits = jnp.zeros((LANE, LANE), jnp.float32)
        for b in range(count):
            hits += (names[b] == target).astype(jnp.float32)
        select[d * LANE : (d + 1) * LANE, :] = jnp.where(same, hits / count, 0.0).astype(jnp.bfloat16)
    loop_lane = jnp.zeros((1, LANE), jnp.int32)
    for z in range(zones):
        loop_lane = jnp.where(lane_zone == z, loop_ref[z], loop_lane)
    wanted = base + (col // zones) * loops + jnp.broadcast_to(loop_lane, (LANE, LANE))
    loop_pick = ((row == wanted) & (col < base)).astype(jnp.float32).astype(jnp.bfloat16)

    loop_of = [loop_ref[z] for z in range(zones)]
    slots = cols - 1
    floor_slots = floors - 1
    sends = []
    for step in range(ITERS):
        source = plan_ref if step == 0 else control
        shares = jnp.zeros((SUB, LANE), jnp.float32)
        tile = jnp.zeros((SUB, LANE), jnp.float32)
        loads = jnp.zeros((SUB, LANE), jnp.float32)
        for z in range(zones):
            if step == 0 and z % step_zones == 0:
                plant_copies[z // step_zones].wait()
            product = plant[z] * source[z : z + 1, :]
            partial = product[:, :LANE]
            for c in range(1, width // LANE):
                partial += product[:, c * LANE : (c + 1) * LANE]
            sums = jnp.sum(partial, axis=1, keepdims=True)
            for j in range(groups):
                share = jnp.broadcast_to(sums[SUB * j : SUB * (j + 1)], (SUB, LANE))
                first = horizon + SUB * j
                bound = jnp.broadcast_to(sums[first : first + SUB], (SUB, LANE))
                mine = lane == zones * j + z
                shares = jnp.where(mine, share, shares)
                tile = jnp.where(mine, bound, tile)
                loads += jnp.where(lane == base + loops * j + loop_of[z], share, 0.0)
        tile = tile + loads
        message[step] = tile
        if step == 0:
            pl.semaphore_wait(barrier, slots + floor_slots)
        for d in range(1, cols):
            copy = pltpu.make_async_remote_copy(
                src_ref=message.at[step],
                dst_ref=heard.at[step, d - 1],
                send_sem=send_sem.at[step, d - 1],
                recv_sem=recv_sem.at[step, d - 1],
                device_id=zone_peers[d - 1],
                device_id_type=MESH,
            )
            copy.start()
            sends.append(copy)
        for copy in sends[len(sends) - slots :]:
            copy.wait_recv()
        floor_tile = tile
        for d in range(slots):
            floor_tile += heard[step, d]
        floor_message[step] = floor_tile
        floor_sends = []
        for d in range(1, floors):
            copy = pltpu.make_async_remote_copy(
                src_ref=floor_message.at[step],
                dst_ref=floor_heard.at[step, d - 1],
                send_sem=floor_send_sem.at[step, d - 1],
                recv_sem=floor_recv_sem.at[step, d - 1],
                device_id=floor_peers[d - 1],
                device_id_type=MESH,
            )
            copy.start()
            floor_sends.append(copy)
        everyone = jnp.concatenate([tile] + [heard[step, d] for d in range(slots)], axis=1)
        near = exact_dot(everyone, select[...])
        here = jnp.where(lane < base, tile, 0.0)
        target_bound = (here + near) * 0.5 - mult
        mult = mult + (here - near) * 0.5
        for copy in floor_sends:
            copy.wait_recv()
        sends += floor_sends
        total = floor_tile
        for d in range(floor_slots):
            total += floor_heard[step, d]
        excess = jnp.where(is_load, (total - demand) * (loops / zones_all), 0.0)
        target_share = shares - exact_dot(excess + price, loop_pick)
        price = price + excess
        for z in range(zones):
            if step == 0 and z % step_zones == 0:
                factor_copies[z // step_zones].wait()
            total_z = jnp.zeros((SUB, width), jnp.float32)
            for half, target in enumerate((target_share, target_bound)):
                for j in range(groups):
                    at = zones * j + z
                    column = jnp.broadcast_to(target[:, at : at + 1], (SUB, width))
                    first = half * horizon + SUB * j
                    total_z += factor[z, first : first + SUB, :] * column
            result = 0.8 * jnp.sum(total_z, axis=0, keepdims=True) - offset_ref[z : z + 1, :]
            if step == ITERS - 1:
                control_out[z : z + 1, :] = result
            else:
                control[z : z + 1, :] = result
    price_out[...] = unpack(price, loops, base)
    mult_out[...] = unpack(mult, zones, 0)
    for copy in sends:
        copy.wait_send()


def hand_over(*refs):
    for source, target in zip(refs[:3], refs[3:]):
        target[...] = source[...]


def solution(mesh):
    floors, cols = mesh.shape["floor"], mesh.shape["zone"]

    def local(factor, plant, offset, plan, demand, price, mult, near, loop):
        zones = plan.shape[0]
        assert (zones + loop_count(demand)) * demand.shape[1] // SUB <= LANE
        vmem = pl.BlockSpec(memory_space=pltpu.VMEM)
        hbm = pl.BlockSpec(memory_space=pltpu.HBM)
        dma = pltpu.SemaphoreType.DMA
        tile = (SUB, LANE)
        results = pl.pallas_call(
            functools.partial(kernel, floors, cols, zones * floors * cols),
            out_shape=tuple(pltpu.VMEM(x.shape, x.dtype) for x in (plan, price, mult)),
            in_specs=[hbm] * 9,
            out_specs=(vmem, vmem, vmem),
            scratch_shapes=[
                pltpu.VMEM(factor.shape, jnp.float32),
                pltpu.VMEM(plant.shape, jnp.float32),
                pltpu.VMEM(plan.shape, jnp.float32),
                pltpu.VMEM((cols * LANE, LANE), jnp.bfloat16),
                pltpu.VMEM((ITERS,) + tile, jnp.float32),
                pltpu.VMEM((ITERS, cols - 1) + tile, jnp.float32),
                pltpu.VMEM((ITERS,) + tile, jnp.float32),
                pltpu.VMEM((ITERS, floors - 1) + tile, jnp.float32),
                pltpu.VMEM(offset.shape, jnp.float32),
                pltpu.VMEM(plan.shape, jnp.float32),
                pltpu.VMEM(demand.shape, jnp.float32),
                pltpu.VMEM(price.shape, jnp.float32),
                pltpu.VMEM(mult.shape, jnp.float32),
                pltpu.SMEM(near.shape[::-1], jnp.int32),
                pltpu.SMEM(loop.shape, jnp.int32),
                dma((7,)),
                dma((CHUNKS,)),
                dma((CHUNKS,)),
                dma((ITERS, cols - 1)),
                dma((ITERS, cols - 1)),
                dma((ITERS, floors - 1)),
                dma((ITERS, floors - 1)),
            ],
            compiler_params=pltpu.CompilerParams(
                collective_id=0, has_side_effects=True
            ),
        )(*(
            pltpu.with_memory_space_constraint(x, pltpu.HBM)
            for x in (factor, plant, offset, plan, demand, price, mult, near.T, loop)
        ))
        return pl.pallas_call(
            hand_over,
            out_shape=tuple(jax.ShapeDtypeStruct(x.shape, x.dtype) for x in results),
            in_specs=[vmem] * 3,
            out_specs=(vmem,) * 3,
            compiler_params=pltpu.CompilerParams(vmem_limit_bytes=2**20),
        )(*results)

    def loop_count(demand):
        return demand.shape[0]

    both = ("floor", "zone")
    placed = (
        P(both, None, None), P(both, None, None), P(both, None), P(both, None),
        P(), P(), P(both, None), P(both, None), P(both),
    )
    return jax.shard_map(
        local,
        mesh=mesh,
        in_specs=placed,
        out_specs=(P(both, None), P(), P(both, None)),
        check_vma=False,
    )
```

```python
import functools

import jax
import jax.numpy as jnp
from jax import lax
from jax.experimental import pallas as pl
from jax.experimental.pallas import tpu as pltpu
from jax.sharding import PartitionSpec as P

ITERS = 2
MESH = pl.DeviceIdType.MESH
SUB, LANE = 8, 128
CHUNKS = 4
PER_ROW = 4


def pieces(x):
    high = x.astype(jnp.bfloat16)
    rest = x - high.astype(jnp.float32)
    mid = rest.astype(jnp.bfloat16)
    low = rest - mid.astype(jnp.float32)
    zero = jnp.zeros_like(low)
    return jnp.concatenate(
        [high.astype(jnp.float32), mid.astype(jnp.float32), low, zero], axis=0
    ).astype(jnp.bfloat16)


def exact_dot(x, picks):
    parts = jnp.dot(pieces(x), picks, preferred_element_type=jnp.float32)
    return parts[:SUB] + parts[SUB : 2 * SUB] + parts[2 * SUB : 3 * SUB]


def kernel(
    floors,
    cols,
    zones_all,
    factor_ref,
    plant_ref,
    offset_hbm,
    plan_hbm,
    demand_hbm,
    price_hbm,
    mult_hbm,
    near_hbm,
    loop_hbm,
    control_out,
    price_out,
    mult_out,
    factor,
    plant,
    control,
    select,
    message,
    heard,
    brief,
    far_heard,
    offset_ref,
    plan_ref,
    demand_ref,
    price_ref,
    mult_ref,
    near_ref,
    loop_ref,
    small_sem,
    plant_sem,
    factor_sem,
    send_sem,
    recv_sem,
    far_send_sem,
    far_recv_sem,
):
    zones, rows, width = plant.shape
    horizon = rows // 2
    groups = horizon // SUB
    loops = demand_ref.shape[0]
    base = groups * zones
    my_floor, me = lax.axis_index("floor"), lax.axis_index("zone")

    step_zones = zones // CHUNKS
    plant_copies, factor_copies = [], []
    for i in range(CHUNKS):
        part = pl.ds(i * step_zones, step_zones)
        plant_copies.append(pltpu.make_async_copy(plant_ref.at[part], plant.at[part], plant_sem.at[i]))
        factor_copies.append(
            pltpu.make_async_copy(factor_ref.at[part], factor.at[part], factor_sem.at[i])
        )
    sources = (loop_hbm, near_hbm, mult_hbm, demand_hbm, price_hbm, plan_hbm, offset_hbm)
    targets = (loop_ref, near_ref, mult_ref, demand_ref, price_ref, plan_ref, offset_ref)
    small = [
        pltpu.make_async_copy(source, target, small_sem.at[i])
        for i, (source, target) in enumerate(zip(sources, targets))
    ]
    for copy in small + plant_copies + factor_copies:
        copy.start()

    order = sorted(range(cols), key=lambda d: -min(d, cols - d))
    zone_peers = [(my_floor, lax.rem(me + d, cols)) for d in order[:-1]]
    far_peers = [
        (lax.rem(my_floor + f, floors), lax.rem(me + d, cols)) for f in range(1, floors) for d in order
    ]
    barrier = pltpu.get_barrier_semaphore()
    for peer in zone_peers + far_peers:
        pl.semaphore_signal(barrier, inc=1, device_id=peer, device_id_type=MESH)

    lane = lax.broadcasted_iota(jnp.int32, (SUB, LANE), 1)

    def pack(x, start):
        count = x.shape[0]
        row = lax.broadcasted_iota(jnp.int32, (count, LANE), 0)
        col = lax.broadcasted_iota(jnp.int32, (count, LANE), 1) - start
        inside = (col >= 0) & (col < groups * count)
        spread = ((lax.rem(jnp.maximum(col, 0), count) == row) & inside).astype(jnp.float32)
        wide = lax.dot_general(
            x, spread, (((0,), (0,)), ((), ())),
            precision=lax.Precision.HIGHEST, preferred_element_type=jnp.float32,
        )
        out = jnp.zeros((SUB, LANE), jnp.float32)
        for j in range(groups):
            first = start + count * j
            mine = (lane >= first) & (lane < first + count)
            out = jnp.where(mine, wide[SUB * j : SUB * (j + 1)], out)
        return out

    def unpack(tile, count, start):
        row = lax.broadcasted_iota(jnp.int32, (count, LANE), 0)
        col = lax.broadcasted_iota(jnp.int32, (count, LANE), 1) - start
        inside = (col >= 0) & (col < groups * count)
        spread = ((lax.rem(jnp.maximum(col, 0), count) == row) & inside).astype(jnp.float32)
        parts = []
        for j in range(groups):
            first = start + count * j
            mine = (lane >= first) & (lane < first + count)
            parts.append(jnp.where(mine, tile, 0.0))
        tall = jnp.concatenate(parts, axis=0)
        return lax.dot_general(
            spread, tall, (((1,), (1,)), ((), ())),
            precision=lax.Precision.HIGHEST, preferred_element_type=jnp.float32,
        )

    is_load = (lane >= base) & (lane < base + groups * loops)
    for copy in small:
        copy.wait()
    demand = pack(demand_ref[...], base)
    price = pack(price_ref[...], base)
    mult = pack(mult_ref[...], 0)

    row = lax.broadcasted_iota(jnp.int32, (LANE, LANE), 0)
    col = lax.broadcasted_iota(jnp.int32, (LANE, LANE), 1)
    wide_lane = lax.broadcasted_iota(jnp.int32, (1, LANE), 1)
    lane_zone = lax.rem(wide_lane, zones)
    same = (row // zones == col // zones) & (row < base) & (col < base)
    count = near_ref.shape[0]
    names = []
    for b in range(count):
        value = jnp.zeros((1, LANE), jnp.int32)
        for z in range(zones):
            value = jnp.where(lane_zone == z, near_ref[b, z], value)
        names.append(jnp.broadcast_to(value, (LANE, LANE)))
    inner = lax.rem(row, zones)
    for d in range(cols):
        owner = lax.rem(me - d + cols, cols)
        target = inner + owner * zones
        hits = jnp.zeros((LANE, LANE), jnp.float32)
        for b in range(count):
            hits += (names[b] == target).astype(jnp.float32)
        select[d * LANE : (d + 1) * LANE, :] = jnp.where(same, hits / count, 0.0).astype(jnp.bfloat16)
    loop_lane = jnp.zeros((1, LANE), jnp.int32)
    for z in range(zones):
        loop_lane = jnp.where(lane_zone == z, loop_ref[z], loop_lane)
    wanted = base + (col // zones) * loops + jnp.broadcast_to(loop_lane, (LANE, LANE))
    loop_pick = ((row == wanted) & (col < base)).astype(jnp.float32).astype(jnp.bfloat16)

    block = LANE // PER_ROW
    sub = lax.broadcasted_iota(jnp.int32, (SUB, LANE), 0)

    def narrow(tile):
        rolled = tile
        for q in range(1, PER_ROW):
            rolled = jnp.where(lax.rem(sub, PER_ROW) == q, pltpu.roll(tile, block * q, 1), rolled)
        return jnp.concatenate(
            [
                jnp.sum(rolled[PER_ROW * r : PER_ROW * (r + 1)], axis=0, keepdims=True)
                for r in range(SUB // PER_ROW)
            ],
            axis=0,
        )

    def widen(pair):
        spread = jnp.concatenate(
            [
                jnp.broadcast_to(pair[r : r + 1], (PER_ROW, LANE))
                for r in range(SUB // PER_ROW)
            ],
            axis=0,
        )
        out = spread
        for q in range(1, PER_ROW):
            out = jnp.where(lax.rem(sub, PER_ROW) == q, pltpu.roll(spread, LANE - block * q, 1), out)
        return out

    loop_of = [loop_ref[z] for z in range(zones)]
    slots = cols - 1
    order_slot = {d: i for i, d in enumerate(order)}
    far_slots = len(far_peers)
    sends = []
    for step in range(ITERS):
        source = plan_ref if step == 0 else control
        shares = jnp.zeros((SUB, LANE), jnp.float32)
        tile = jnp.zeros((SUB, LANE), jnp.float32)
        loads = jnp.zeros((SUB, LANE), jnp.float32)
        for z in range(zones):
            if step == 0 and z % step_zones == 0:
                plant_copies[z // step_zones].wait()
            product = plant[z] * source[z : z + 1, :]
            partial = product[:, :LANE]
            for c in range(1, width // LANE):
                partial += product[:, c * LANE : (c + 1) * LANE]
            sums = jnp.sum(partial, axis=1, keepdims=True)
            for j in range(groups):
                share = jnp.broadcast_to(sums[SUB * j : SUB * (j + 1)], (SUB, LANE))
                first = horizon + SUB * j
                bound = jnp.broadcast_to(sums[first : first + SUB], (SUB, LANE))
                mine = lane == zones * j + z
                shares = jnp.where(mine, share, shares)
                tile = jnp.where(mine, bound, tile)
                loads += jnp.where(lane == base + loops * j + loop_of[z], share, 0.0)
        tile = tile + loads
        brief[step] = narrow(loads)
        message[step] = tile
        if step == 0:
            pl.semaphore_wait(barrier, slots + far_slots)
        far_sends = []
        for i, peer in enumerate(far_peers):
            copy = pltpu.make_async_remote_copy(
                src_ref=brief.at[step],
                dst_ref=far_heard.at[step, i],
                send_sem=far_send_sem.at[step, i],
                recv_sem=far_recv_sem.at[step, i],
                device_id=peer,
                device_id_type=MESH,
            )
            copy.start()
            far_sends.append(copy)
        for d in range(1, cols):
            copy = pltpu.make_async_remote_copy(
                src_ref=message.at[step],
                dst_ref=heard.at[step, d - 1],
                send_sem=send_sem.at[step, d - 1],
                recv_sem=recv_sem.at[step, d - 1],
                device_id=zone_peers[d - 1],
                device_id_type=MESH,
            )
            copy.start()
            sends.append(copy)
        for copy in sends[len(sends) - slots :]:
            copy.wait_recv()
        total = tile
        for d in range(slots):
            total += heard[step, d]
        everyone = jnp.concatenate([tile] + [heard[step, order_slot[d]] for d in range(1, cols)], axis=1)
        near = exact_dot(everyone, select[...])
        here = jnp.where(lane < base, tile, 0.0)
        target_bound = (here + near) * 0.5 - mult
        mult = mult + (here - near) * 0.5
        for copy in far_sends:
            copy.wait_recv()
        sends += far_sends
        far = far_heard[step, 0]
        for i in range(1, far_slots):
            far += far_heard[step, i]
        total += widen(far)
        excess = jnp.where(is_load, (total - demand) * (loops / zones_all), 0.0)
        target_share = shares - exact_dot(excess + price, loop_pick)
        price = price + excess
        for z in range(zones):
            if step == 0 and z % step_zones == 0:
                factor_copies[z // step_zones].wait()
            total_z = jnp.zeros((SUB, width), jnp.float32)
            for half, target in enumerate((target_share, target_bound)):
                for j in range(groups):
                    at = zones * j + z
                    column = jnp.broadcast_to(target[:, at : at + 1], (SUB, width))
                    first = half * horizon + SUB * j
                    total_z += factor[z, first : first + SUB, :] * column
            result = 0.8 * jnp.sum(total_z, axis=0, keepdims=True) - offset_ref[z : z + 1, :]
            if step == ITERS - 1:
                control_out[z : z + 1, :] = result
            else:
                control[z : z + 1, :] = result
    price_out[...] = unpack(price, loops, base)
    mult_out[...] = unpack(mult, zones, 0)
    for copy in sends:
        copy.wait_send()


def hand_over(*refs):
    for source, target in zip(refs[:3], refs[3:]):
        target[...] = source[...]


def solution(mesh):
    floors, cols = mesh.shape["floor"], mesh.shape["zone"]

    def local(factor, plant, offset, plan, demand, price, mult, near, loop):
        zones = plan.shape[0]
        assert (zones + loop_count(demand)) * demand.shape[1] // SUB <= LANE
        vmem = pl.BlockSpec(memory_space=pltpu.VMEM)
        hbm = pl.BlockSpec(memory_space=pltpu.HBM)
        dma = pltpu.SemaphoreType.DMA
        tile = (SUB, LANE)
        far = (floors - 1) * cols
        results = pl.pallas_call(
            functools.partial(kernel, floors, cols, zones * floors * cols),
            out_shape=tuple(pltpu.VMEM(x.shape, x.dtype) for x in (plan, price, mult)),
            in_specs=[hbm] * 9,
            out_specs=(vmem, vmem, vmem),
            scratch_shapes=[
                pltpu.VMEM(factor.shape, jnp.float32),
                pltpu.VMEM(plant.shape, jnp.float32),
                pltpu.VMEM(plan.shape, jnp.float32),
                pltpu.VMEM((cols * LANE, LANE), jnp.bfloat16),
                pltpu.VMEM((ITERS,) + tile, jnp.float32),
                pltpu.VMEM((ITERS, cols - 1) + tile, jnp.float32),
                pltpu.VMEM((ITERS, SUB // PER_ROW, LANE), jnp.float32),
                pltpu.VMEM((ITERS, far, SUB // PER_ROW, LANE), jnp.float32),
                pltpu.VMEM(offset.shape, jnp.float32),
                pltpu.VMEM(plan.shape, jnp.float32),
                pltpu.VMEM(demand.shape, jnp.float32),
                pltpu.VMEM(price.shape, jnp.float32),
                pltpu.VMEM(mult.shape, jnp.float32),
                pltpu.SMEM(near.shape[::-1], jnp.int32),
                pltpu.SMEM(loop.shape, jnp.int32),
                dma((7,)),
                dma((CHUNKS,)),
                dma((CHUNKS,)),
                dma((ITERS, cols - 1)),
                dma((ITERS, cols - 1)),
                dma((ITERS, far)),
                dma((ITERS, far)),
            ],
            compiler_params=pltpu.CompilerParams(
                collective_id=0, has_side_effects=True
            ),
        )(*(
            pltpu.with_memory_space_constraint(x, pltpu.HBM)
            for x in (factor, plant, offset, plan, demand, price, mult, near.T, loop)
        ))
        return pl.pallas_call(
            hand_over,
            out_shape=tuple(jax.ShapeDtypeStruct(x.shape, x.dtype) for x in results),
            in_specs=[vmem] * 3,
            out_specs=(vmem,) * 3,
            compiler_params=pltpu.CompilerParams(vmem_limit_bytes=2**20),
        )(*results)

    def loop_count(demand):
        return demand.shape[0]

    both = ("floor", "zone")
    placed = (
        P(both, None, None), P(both, None, None), P(both, None), P(both, None),
        P(), P(), P(both, None), P(both, None), P(both),
    )
    return jax.shard_map(
        local,
        mesh=mesh,
        in_specs=placed,
        out_specs=(P(both, None), P(), P(both, None)),
        check_vma=False,
    )
```

```python
import functools

import jax
import jax.numpy as jnp
from jax import lax
from jax.experimental import pallas as pl
from jax.experimental.pallas import tpu as pltpu
from jax.sharding import PartitionSpec as P

ITERS = 2
MESH = pl.DeviceIdType.MESH
SUB, LANE = 8, 128
CHUNKS = 4
PER_ROW = 4


def pieces(x):
    high = x.astype(jnp.bfloat16)
    rest = x - high.astype(jnp.float32)
    mid = rest.astype(jnp.bfloat16)
    low = rest - mid.astype(jnp.float32)
    zero = jnp.zeros_like(low)
    return jnp.concatenate(
        [high.astype(jnp.float32), mid.astype(jnp.float32), low, zero], axis=0
    ).astype(jnp.bfloat16)


def exact_dot(x, picks):
    parts = jnp.dot(pieces(x), picks, preferred_element_type=jnp.float32)
    return parts[:SUB] + parts[SUB : 2 * SUB] + parts[2 * SUB : 3 * SUB]


def kernel(
    floors,
    cols,
    zones_all,
    factor_ref,
    plant_ref,
    offset_hbm,
    plan_hbm,
    demand_hbm,
    price_hbm,
    mult_hbm,
    near_hbm,
    loop_hbm,
    control_out,
    price_out,
    mult_out,
    factor,
    plant,
    control,
    select,
    bound_part,
    message,
    heard,
    brief,
    far_heard,
    offset_ref,
    plan_ref,
    demand_ref,
    price_ref,
    mult_ref,
    near_ref,
    loop_ref,
    small_sem,
    plant_sem,
    factor_sem,
    send_sem,
    recv_sem,
    far_send_sem,
    far_recv_sem,
):
    zones, rows, width = plant.shape
    horizon = rows // 2
    groups = horizon // SUB
    loops = demand_ref.shape[0]
    base = groups * zones
    my_floor, me = lax.axis_index("floor"), lax.axis_index("zone")

    step_zones = zones // CHUNKS
    plant_copies, factor_copies = [], []
    for i in range(CHUNKS):
        part = pl.ds(i * step_zones, step_zones)
        plant_copies.append(pltpu.make_async_copy(plant_ref.at[part], plant.at[part], plant_sem.at[i]))
        factor_copies.append(
            pltpu.make_async_copy(factor_ref.at[part], factor.at[part], factor_sem.at[i])
        )
    sources = (loop_hbm, near_hbm, mult_hbm, demand_hbm, price_hbm, plan_hbm, offset_hbm)
    targets = (loop_ref, near_ref, mult_ref, demand_ref, price_ref, plan_ref, offset_ref)
    small = [
        pltpu.make_async_copy(source, target, small_sem.at[i])
        for i, (source, target) in enumerate(zip(sources, targets))
    ]
    for copy in small + plant_copies:
        copy.start()

    order = sorted(range(cols), key=lambda d: -min(d, cols - d))
    zone_peers = [(my_floor, lax.rem(me + d, cols)) for d in order[:-1]]
    far_peers = [
        (lax.rem(my_floor + f, floors), lax.rem(me + d, cols)) for f in range(1, floors) for d in order
    ]
    barrier = pltpu.get_barrier_semaphore()
    for peer in far_peers + zone_peers:
        pl.semaphore_signal(barrier, inc=1, device_id=peer, device_id_type=MESH)
    for copy in factor_copies:
        copy.start()

    lane = lax.broadcasted_iota(jnp.int32, (SUB, LANE), 1)

    def pack(x, start):
        count = x.shape[0]
        row = lax.broadcasted_iota(jnp.int32, (count, LANE), 0)
        col = lax.broadcasted_iota(jnp.int32, (count, LANE), 1) - start
        inside = (col >= 0) & (col < groups * count)
        spread = ((lax.rem(jnp.maximum(col, 0), count) == row) & inside).astype(jnp.float32)
        wide = lax.dot_general(
            x, spread, (((0,), (0,)), ((), ())),
            precision=lax.Precision.HIGHEST, preferred_element_type=jnp.float32,
        )
        out = jnp.zeros((SUB, LANE), jnp.float32)
        for j in range(groups):
            first = start + count * j
            mine = (lane >= first) & (lane < first + count)
            out = jnp.where(mine, wide[SUB * j : SUB * (j + 1)], out)
        return out

    def unpack(tile, count, start):
        row = lax.broadcasted_iota(jnp.int32, (count, LANE), 0)
        col = lax.broadcasted_iota(jnp.int32, (count, LANE), 1) - start
        inside = (col >= 0) & (col < groups * count)
        spread = ((lax.rem(jnp.maximum(col, 0), count) == row) & inside).astype(jnp.float32)
        parts = []
        for j in range(groups):
            first = start + count * j
            mine = (lane >= first) & (lane < first + count)
            parts.append(jnp.where(mine, tile, 0.0))
        tall = jnp.concatenate(parts, axis=0)
        return lax.dot_general(
            spread, tall, (((1,), (1,)), ((), ())),
            precision=lax.Precision.HIGHEST, preferred_element_type=jnp.float32,
        )

    is_load = (lane >= base) & (lane < base + groups * loops)
    for copy in small:
        copy.wait()
    demand = pack(demand_ref[...], base)
    price = pack(price_ref[...], base)
    mult = pack(mult_ref[...], 0)

    row = lax.broadcasted_iota(jnp.int32, (LANE, LANE), 0)
    col = lax.broadcasted_iota(jnp.int32, (LANE, LANE), 1)
    wide_lane = lax.broadcasted_iota(jnp.int32, (1, LANE), 1)
    lane_zone = lax.rem(wide_lane, zones)
    same = (row // zones == col // zones) & (row < base) & (col < base)
    count = near_ref.shape[0]
    names = []
    for b in range(count):
        value = jnp.zeros((1, LANE), jnp.int32)
        for z in range(zones):
            value = jnp.where(lane_zone == z, near_ref[b, z], value)
        names.append(jnp.broadcast_to(value, (LANE, LANE)))
    inner = lax.rem(row, zones)
    for d in range(cols):
        owner = lax.rem(me - d + cols, cols)
        target = inner + owner * zones
        hits = jnp.zeros((LANE, LANE), jnp.float32)
        for b in range(count):
            hits += (names[b] == target).astype(jnp.float32)
        select[d * LANE : (d + 1) * LANE, :] = jnp.where(same, hits / count, 0.0).astype(jnp.bfloat16)
    loop_lane = jnp.zeros((1, LANE), jnp.int32)
    for z in range(zones):
        loop_lane = jnp.where(lane_zone == z, loop_ref[z], loop_lane)
    wanted = base + (col // zones) * loops + jnp.broadcast_to(loop_lane, (LANE, LANE))
    loop_pick = ((row == wanted) & (col < base)).astype(jnp.float32).astype(jnp.bfloat16)

    block = LANE // PER_ROW
    sub = lax.broadcasted_iota(jnp.int32, (SUB, LANE), 0)

    def narrow(tile):
        rolled = tile
        for q in range(1, PER_ROW):
            rolled = jnp.where(lax.rem(sub, PER_ROW) == q, pltpu.roll(tile, block * q, 1), rolled)
        return jnp.concatenate(
            [
                jnp.sum(rolled[PER_ROW * r : PER_ROW * (r + 1)], axis=0, keepdims=True)
                for r in range(SUB // PER_ROW)
            ],
            axis=0,
        )

    def widen(pair):
        spread = jnp.concatenate(
            [
                jnp.broadcast_to(pair[r : r + 1], (PER_ROW, LANE))
                for r in range(SUB // PER_ROW)
            ],
            axis=0,
        )
        out = spread
        for q in range(1, PER_ROW):
            out = jnp.where(lax.rem(sub, PER_ROW) == q, pltpu.roll(spread, LANE - block * q, 1), out)
        return out

    def half_sum(target, z, half):
        out = jnp.zeros((SUB, width), jnp.float32)
        for j in range(groups):
            at = zones * j + z
            column = jnp.broadcast_to(target[:, at : at + 1], (SUB, width))
            first = half * horizon + SUB * j
            out += factor[z, first : first + SUB, :] * column
        return out

    loop_of = [loop_ref[z] for z in range(zones)]
    slots = cols - 1
    order_slot = {d: i for i, d in enumerate(order)}
    far_slots = len(far_peers)
    sends = []
    for step in range(ITERS):
        source = plan_ref if step == 0 else control
        shares = jnp.zeros((SUB, LANE), jnp.float32)
        tile = jnp.zeros((SUB, LANE), jnp.float32)
        loads = jnp.zeros((SUB, LANE), jnp.float32)
        for z in range(zones):
            if step == 0 and z % step_zones == 0:
                plant_copies[z // step_zones].wait()
            product = plant[z] * source[z : z + 1, :]
            partial = product[:, :LANE]
            for c in range(1, width // LANE):
                partial += product[:, c * LANE : (c + 1) * LANE]
            sums = jnp.sum(partial, axis=1, keepdims=True)
            for j in range(groups):
                share = jnp.broadcast_to(sums[SUB * j : SUB * (j + 1)], (SUB, LANE))
                first = horizon + SUB * j
                bound = jnp.broadcast_to(sums[first : first + SUB], (SUB, LANE))
                mine = lane == zones * j + z
                shares = jnp.where(mine, share, shares)
                tile = jnp.where(mine, bound, tile)
                loads += jnp.where(lane == base + loops * j + loop_of[z], share, 0.0)
        tile = tile + loads
        brief[step] = narrow(loads)
        message[step] = tile
        if step == 0:
            pl.semaphore_wait(barrier, slots + far_slots)
        far_sends = []
        for i, peer in enumerate(far_peers):
            copy = pltpu.make_async_remote_copy(
                src_ref=brief.at[step],
                dst_ref=far_heard.at[step, i],
                send_sem=far_send_sem.at[step, i],
                recv_sem=far_recv_sem.at[step, i],
                device_id=peer,
                device_id_type=MESH,
            )
            copy.start()
            far_sends.append(copy)
        for d in range(1, cols):
            copy = pltpu.make_async_remote_copy(
                src_ref=message.at[step],
                dst_ref=heard.at[step, d - 1],
                send_sem=send_sem.at[step, d - 1],
                recv_sem=recv_sem.at[step, d - 1],
                device_id=zone_peers[d - 1],
                device_id_type=MESH,
            )
            copy.start()
            sends.append(copy)
        for copy in sends[len(sends) - slots :]:
            copy.wait_recv()
        total = tile
        for d in range(slots):
            total += heard[step, d]
        everyone = jnp.concatenate([tile] + [heard[step, order_slot[d]] for d in range(1, cols)], axis=1)
        near = exact_dot(everyone, select[...])
        here = jnp.where(lane < base, tile, 0.0)
        target_bound = (here + near) * 0.5 - mult
        mult = mult + (here - near) * 0.5
        for z in range(zones):
            if step == 0 and z % step_zones == 0:
                factor_copies[z // step_zones].wait()
            bound_part[z] = half_sum(target_bound, z, 1)
        for copy in far_sends:
            copy.wait_recv()
        sends += far_sends
        far = far_heard[step, 0]
        for i in range(1, far_slots):
            far += far_heard[step, i]
        total += widen(far)
        excess = jnp.where(is_load, (total - demand) * (loops / zones_all), 0.0)
        target_share = shares - exact_dot(excess + price, loop_pick)
        price = price + excess
        for z in range(zones):
            result_sum = bound_part[z] + half_sum(target_share, z, 0)
            result = 0.8 * jnp.sum(result_sum, axis=0, keepdims=True) - offset_ref[z : z + 1, :]
            if step == ITERS - 1:
                control_out[z : z + 1, :] = result
            else:
                control[z : z + 1, :] = result
    price_out[...] = unpack(price, loops, base)
    mult_out[...] = unpack(mult, zones, 0)
    for copy in sends:
        copy.wait_send()


def hand_over(*refs):
    for source, target in zip(refs[:3], refs[3:]):
        target[...] = source[...]


def solution(mesh):
    floors, cols = mesh.shape["floor"], mesh.shape["zone"]

    def local(factor, plant, offset, plan, demand, price, mult, near, loop):
        zones = plan.shape[0]
        assert (zones + loop_count(demand)) * demand.shape[1] // SUB <= LANE
        vmem = pl.BlockSpec(memory_space=pltpu.VMEM)
        hbm = pl.BlockSpec(memory_space=pltpu.HBM)
        dma = pltpu.SemaphoreType.DMA
        tile = (SUB, LANE)
        far = (floors - 1) * cols
        results = pl.pallas_call(
            functools.partial(kernel, floors, cols, zones * floors * cols),
            out_shape=tuple(pltpu.VMEM(x.shape, x.dtype) for x in (plan, price, mult)),
            in_specs=[hbm] * 9,
            out_specs=(vmem, vmem, vmem),
            scratch_shapes=[
                pltpu.VMEM(factor.shape, jnp.float32),
                pltpu.VMEM(plant.shape, jnp.float32),
                pltpu.VMEM(plan.shape, jnp.float32),
                pltpu.VMEM((cols * LANE, LANE), jnp.bfloat16),
                pltpu.VMEM((zones, SUB, factor.shape[2]), jnp.float32),
                pltpu.VMEM((ITERS,) + tile, jnp.float32),
                pltpu.VMEM((ITERS, cols - 1) + tile, jnp.float32),
                pltpu.VMEM((ITERS, SUB // PER_ROW, LANE), jnp.float32),
                pltpu.VMEM((ITERS, far, SUB // PER_ROW, LANE), jnp.float32),
                pltpu.VMEM(offset.shape, jnp.float32),
                pltpu.VMEM(plan.shape, jnp.float32),
                pltpu.VMEM(demand.shape, jnp.float32),
                pltpu.VMEM(price.shape, jnp.float32),
                pltpu.VMEM(mult.shape, jnp.float32),
                pltpu.SMEM(near.shape[::-1], jnp.int32),
                pltpu.SMEM(loop.shape, jnp.int32),
                dma((7,)),
                dma((CHUNKS,)),
                dma((CHUNKS,)),
                dma((ITERS, cols - 1)),
                dma((ITERS, cols - 1)),
                dma((ITERS, far)),
                dma((ITERS, far)),
            ],
            compiler_params=pltpu.CompilerParams(
                collective_id=0, has_side_effects=True
            ),
        )(*(
            pltpu.with_memory_space_constraint(x, pltpu.HBM)
            for x in (factor, plant, offset, plan, demand, price, mult, near.T, loop)
        ))
        return pl.pallas_call(
            hand_over,
            out_shape=tuple(jax.ShapeDtypeStruct(x.shape, x.dtype) for x in results),
            in_specs=[vmem] * 3,
            out_specs=(vmem,) * 3,
            compiler_params=pltpu.CompilerParams(vmem_limit_bytes=2**20),
        )(*results)

    def loop_count(demand):
        return demand.shape[0]

    both = ("floor", "zone")
    placed = (
        P(both, None, None), P(both, None, None), P(both, None), P(both, None),
        P(), P(), P(both, None), P(both, None), P(both),
    )
    return jax.shard_map(
        local,
        mesh=mesh,
        in_specs=placed,
        out_specs=(P(both, None), P(), P(both, None)),
        check_vma=False,
    )
```
